512 devices in a mesh: cfd: 64 (over z_lo, x, core), ac: 8 (over y, z_hi).
Axes of the slice: x: 4, y: 4, z: 16 (z_hi: 2, z_lo: 8; z = z_hi * 8 + z_lo), core: 2. Of those that a mesh axis runs over, the one named last changes fastest.
Arguments:
- surface_raw: bfloat16 [5, 65536, 1024], P(None, ('cfd', 'ac')), may hold values from -6 to 6
- area_normals: bfloat16 [3, 65536], P(None, ('cfd', 'ac')), may hold values from -6 to 6
- kernel_weights: bfloat16 [2, 3, 2048, 65536], P(None, None, None, ('cfd', 'ac')), may hold values from -0.0390625 to 0.0390625
- block_map: int32 [8, 64, 64], P('ac', 'cfd'), may hold values from 0 to 63, as said below
- band_observers: int32 [16, 128], replicated, may hold values from 0 to 2047, as said below
- band_lags: int32 [16], replicated, may hold values from 0 to 511
Outputs:
- acoustic: float32 [2048, 512], P('cfd', 'ac')
The draws below stay inside these ranges and needn't reach their ends.
Inputs may be any that keep to these rules, and one draw needn't show every extreme that they name: block_map[j, s, :] is a permutation of 0 to 63 for every j and s. `band_observers`: every observer appears exactly once.
All inputs are finite; a program needn't handle non-finite values.
Results may differ from the reference program's by a relative error of at most 0.0042.
Values may be sent and summed in bfloat16 or wider, within the bound.
A program may use at most 64 MiB of HBM per device.

```python
import jax
import jax.numpy as jnp
from jax import lax

OBS = 2048
BANDS = 16
OBS_BAND = 128
TAPS = 2
BLOCK = 2
FACES = 65536
WINDOW = 1024
OUT_STEPS = 512
N_CFD = 64
N_AC = 8


def draw_band_observers(key, part):
    shuffled = jax.random.permutation(jax.random.fold_in(key, 11), OBS)
    return shuffled.astype(jnp.int32).reshape(BANDS, OBS // BANDS)


def draw_block_map(key, part):
    key_list = jax.random.split(jax.random.fold_in(key, 23), N_AC * N_CFD)
    orders = jax.vmap(lambda single_key: jax.random.permutation(single_key, N_CFD))(key_list)
    return orders.astype(jnp.int32).reshape(N_AC, N_CFD, N_CFD)


def set_ends(entries, stream_key, low, top_value):
    longest = entries.shape.index(max(entries.shape))
    spots = []
    for shift in (0, 1):
        where = [jax.random.randint(jax.random.fold_in(stream_key, axis), (), 0, length) for axis, length in enumerate(entries.shape)]
        where[longest] = (where[longest] + shift) % entries.shape[longest]
        spots.append(tuple(where))
    return entries.at[spots[0]].set(low).at[spots[1]].set(top_value)


def spiked(entries, rng, source, target, parts, factor):
    owner, partner = [(jnp.arange(entries.shape[axis_at]) // (entries.shape[axis_at] // parts)).reshape([-1 if axis == axis_at else 1 for axis in range(entries.ndim)]) for axis_at in (source, target)]
    chosen = jax.random.permutation(rng, parts)[partner]
    strong = (owner == chosen) | (owner == (partner + parts // 2) % parts)
    return jnp.where(strong, factor * entries, entries)


def block_scale(rng, shape, pieces, least, high):
    def one(dim, shards_of):
        draws = jax.random.uniform(jax.random.fold_in(jax.random.fold_in(rng, 6), dim), (shards_of,), jnp.float32, least / len(pieces), high / len(pieces))
        return jnp.repeat(jnp.exp(draws), shape[dim] // shards_of).reshape((-1,) + (1,) * (len(shape) - dim - 1))

    factor_of = one(*pieces[0])
    for cut in pieces[1:]:
        factor_of = factor_of * one(*cut)
    return factor_of


def gaussian(rng, dims, width, most, cuts=(), kind=jnp.bfloat16):
    values = width * jax.random.normal(rng, dims, jnp.float32)
    if cuts:
        values = values * block_scale(rng, dims, cuts, -0.22, 0.18)
    return jnp.clip(values, -most, most).astype(kind)


def gaussian_with(key, dims, scale, limit, cuts, heavy, held_as=jnp.bfloat16):
    result = scale * jax.random.normal(key, dims, jnp.float32)
    if cuts:
        result = result * block_scale(key, dims, cuts, -0.22, 0.18)
    return jnp.clip(spiked(result, jax.random.fold_in(key, 3), *heavy), -limit, limit).astype(held_as)


def setup_inputs(seed: int = 0) -> dict:
    seeds = jax.random.split(jax.random.key(seed), 7)
    surface_raw = gaussian(seeds[0], (5, FACES, WINDOW), 1.0, 6.0, ((1, 512),))
    area_normals = gaussian(seeds[1], (3, FACES), 1.0, 6.0, ((1, 512),))
    kernel_weights = gaussian_with(seeds[2], (TAPS, 3, OBS, FACES), (6 * FACES) ** -0.5, 0.0390625, ((3, 512),), (3, 2, 512, 6.0))
    block_map = draw_block_map(jax.random.fold_in(seeds[6], 71), 0)
    band_observers = draw_band_observers(jax.random.fold_in(seeds[6], 71), 0)
    band_lags = set_ends(jax.random.randint(seeds[5], (BANDS,), 0, OUT_STEPS), jax.random.fold_in(seeds[5], 1), 0, OUT_STEPS - 1).astype(jnp.int32)
    return dict(surface_raw=surface_raw, area_normals=area_normals, kernel_weights=kernel_weights, block_map=block_map, band_observers=band_observers, band_lags=band_lags)


def thickness(surface, normals):
    along = surface[2].astype(jnp.float32) * normals[0].astype(jnp.float32)[:, None]
    along = along + surface[3].astype(jnp.float32) * normals[1].astype(jnp.float32)[:, None]
    along = along + surface[4].astype(jnp.float32) * normals[2].astype(jnp.float32)[:, None]
    return (surface[1].astype(jnp.float32) * along).astype(jnp.bfloat16)


def rates(series):
    step = series[:, 1:].astype(jnp.float32) - series[:, :-1].astype(jnp.float32)
    first = jnp.zeros((series.shape[0], 1), jnp.float32)
    return jnp.concatenate([first, step], axis=1).astype(jnp.bfloat16)


def reference(surface_raw, area_normals, kernel_weights, block_map, band_observers, band_lags):
    thick = thickness(surface_raw, area_normals)
    stacked = jnp.stack([thick, surface_raw[0]])
    shaped = stacked.reshape(2, N_CFD, N_AC, N_CFD, BLOCK, WINDOW)
    picks = jnp.transpose(block_map, (1, 0, 2))[None, :, :, :, None, None]
    moved = jnp.take_along_axis(shaped, picks, axis=3)
    moved = jnp.transpose(moved, (0, 3, 2, 1, 4, 5)).reshape(2, FACES, WINDOW)
    sources = jnp.stack([rates(moved[0]), rates(moved[1]), moved[1]])

    def one_band(acoustic, band_index):
        members = band_observers[band_index]
        delay = band_lags[band_index]
        start = (band_index * OBS_BAND).astype(jnp.int32)
        chosen = lax.dynamic_slice_in_dim(kernel_weights, start, OBS_BAND, 2).astype(jnp.float32)
        windows = jnp.stack([lax.dynamic_slice_in_dim(sources, (OUT_STEPS - delay - shift_step).astype(jnp.int32), OUT_STEPS, 2) for shift_step in range(TAPS)]).astype(jnp.float32)
        contribution = jnp.einsum("kcof,kcft->ot", chosen, windows, precision=lax.Precision.HIGHEST)
        return acoustic.at[members].set(contribution), None

    initial = jnp.zeros((OBS, OUT_STEPS), jnp.float32)
    acoustic, _ = lax.scan(one_band, initial, jnp.arange(BANDS, dtype=jnp.int32))
    return acoustic
```

```python
import functools

import jax
import jax.numpy as jnp
from jax import lax
from jax.experimental import pallas as pl
from jax.experimental.pallas import tpu as pltpu
from jax.sharding import PartitionSpec as P

MESH = pl.DeviceIdType.MESH
F32 = jnp.float32
BF16 = jnp.bfloat16


def kernel(
    block_map,
    band_observers,
    band_lags,
    surface,
    normals,
    weights_hbm,
    out,
    face_rows,
    staging,
    arrived,
    weights,
    sources,
    product,
    slots,
    rows_tmp,
    inverse_v,
    inverse,
    core_send,
    core_recv,
    send1,
    recv1,
    send2,
    recv2,
    send3,
    recv3,
    weight_sem,
    inverse_sem,
    face_sems,
    core_sems,
    sems1,
    sems2,
    sems3,
):
    cfd = lax.axis_index("cfd")
    ac = lax.axis_index("ac")
    z_lo = cfd // 8
    x = (cfd // 2) % 4
    core = cfd % 2
    y = ac // 2
    z_hi = ac % 2

    def device(z_lo_=z_lo, x_=x, core_=core, y_=y, z_hi_=z_hi):
        return ((z_lo_ * 4 + x_) * 2 + core_, y_ * 2 + z_hi_)

    weight_copy = pltpu.make_async_copy(weights_hbm, weights, weight_sem)
    weight_copy.start()

    barrier = pltpu.get_barrier_semaphore()

    @pl.loop(1, 64)
    def _(offset):
        pl.semaphore_signal(
            barrier, inc=1, device_id=((cfd + offset) % 64, ac), device_id_type=MESH
        )

    for k in range(1, 4):
        pl.semaphore_signal(
            barrier, inc=1, device_id=device(y_=(y + k) % 4), device_id_type=MESH
        )

    for k in range(8):
        pl.semaphore_signal(
            barrier, inc=1, device_id=device(z_lo_=k, z_hi_=1 - z_hi), device_id_type=MESH
        )

    columns = jnp.transpose(
        jnp.concatenate([normals[...].astype(F32), jnp.zeros((5, 128), F32)], axis=0)
    )
    n0, n1, n2 = columns[:, 0:1], columns[:, 1:2], columns[:, 2:3]
    for tile in range(8):
        lanes = pl.ds(tile * 128, 128)
        along = surface[2, :, lanes].astype(F32) * n0
        along = along + surface[3, :, lanes].astype(F32) * n1
        along = along + surface[4, :, lanes].astype(F32) * n2
        face_rows[0, pl.ds(tile, 128, stride=8), :] = surface[1, :, lanes].astype(F32) * along
        face_rows[1, pl.ds(tile, 128, stride=8), :] = surface[0, :, lanes].astype(F32)

    @pl.loop(0, 64, unroll=4)
    def _(d):
        first = block_map[0, 0, d] * 16
        staging[d, pl.ds(0, 16), :] = face_rows[0, pl.ds(first, 16), :].astype(BF16)
        staging[d, pl.ds(16, 16), :] = face_rows[1, pl.ds(first, 16), :].astype(BF16)

    pl.semaphore_wait(barrier, 74)

    def send_block(dest_z, dest_x, dest_core):
        dest = (dest_z * 4 + dest_x) * 2 + dest_core
        pltpu.make_async_remote_copy(
            src_ref=staging.at[dest],
            dst_ref=arrived.at[cfd],
            send_sem=face_sems.at[0],
            recv_sem=face_sems.at[1],
            device_id=(dest, ac),
            device_id_type=MESH,
        ).start()

    @pl.loop(0, 7)
    def _(step):
        dz = 7 - step
        for sign in (1, -1):
            dest_z = z_lo + sign * dz

            @pl.when((dest_z >= 0) & (dest_z < 8))
            def _():
                for k in range(8):
                    send_block(dest_z, (x + k // 2) % 4, (core + k) % 2)

    for k in range(1, 8):
        send_block(z_lo, (x + k // 2) % 4, (core + k) % 2)
    arrived[cfd] = staging[cfd]

    observer = lax.broadcasted_iota(jnp.int32, (16, 128), 0) * 128 + lax.broadcasted_iota(
        jnp.int32, (16, 128), 1
    )

    def find(band, found):
        for m in range(128):
            found = jnp.where(observer == band_observers[band, m], band * 128 + m, found)
        return found

    inverse_v[...] = lax.fori_loop(0, 16, find, jnp.zeros((16, 128), jnp.int32))
    inverse_copy = pltpu.make_async_copy(inverse_v, inverse, inverse_sem)
    inverse_copy.start()
    product[8] = jnp.zeros((2048, 128), F32)
    weight_copy.wait()
    inverse_copy.wait()

    pltpu.make_async_copy(
        arrived.at[pl.ds(0, 63)], staging.at[pl.ds(0, 63)], face_sems.at[1]
    ).wait()

    for series in range(2):
        for part in range(8):
            tile = arrived[pl.ds(part * 8, 8), pl.ds(series * 16, 16), :].astype(F32)
            face_rows[series, pl.ds(part * 128, 128), :] = tile.reshape(128, 128)
    lane = lax.broadcasted_iota(jnp.int32, (128, 128), 1)
    for series in range(2):
        rolled = None
        step_rolled = None
        for tile in range(8):
            lanes = pl.ds(tile * 128, 128)
            now = face_rows[series, pl.ds(tile, 128, stride=8), :]
            turned = pltpu.roll(now, 1, 1)
            before = jnp.where(lane == 0, now if tile == 0 else rolled, turned)
            rolled = turned
            step = (now - before).astype(BF16).astype(F32)
            step_turned = pltpu.roll(step, 1, 1)
            step_before = jnp.where(
                lane == 0, jnp.zeros_like(step) if tile == 0 else step_rolled, step_turned
            )
            step_rolled = step_turned
            sources[pl.ds(series * 128, 128), lanes] = step.astype(BF16)
            sources[pl.ds((3 + series) * 128, 128), lanes] = step_before.astype(BF16)
            if series == 1:
                sources[pl.ds(2 * 128, 128), lanes] = now.astype(BF16)
                sources[pl.ds(5 * 128, 128), lanes] = before.astype(BF16)

    @pl.loop(0, 4)
    def _(n):
        lanes = pl.ds(pl.multiple_of(n * 256, 256), 256)
        for m in range(2):
            rows = pl.ds(m * 1024, 1024)
            left = jnp.concatenate([weights[kc, rows, :] for kc in range(6)], axis=1)
            both = jnp.dot(left, sources[:, lanes], preferred_element_type=F32)
            product[2 * n, rows, :] = both[:, 0:128]
            product[2 * n + 1, rows, :] = both[:, 128:256]

    @pl.loop(0, 16)
    def _(band):
        start = 512 - band_lags[band]
        tile = lax.div(start, 128)
        within = lax.rem(start, 128)
        turn = lax.rem(128 - within, 128)
        rows = pl.ds(pl.multiple_of(band * 128, 128), 128)
        turned = []
        for j in range(5):
            turned.append(pltpu.roll(product[tile + j, rows, :], turn, 1))
            if j > 0:
                slots[pl.ds(band * 512 + j - 1, 128, stride=4), :] = jnp.where(
                    lane < 128 - within, turned[j - 1], turned[j]
                )

    def gather(block_z, block_x, block_core, buffer):
        first = (block_z * 4 + block_x) * 2 + block_core
        for r in range(32):
            slot = inverse[first // 4, (first % 4) * 32 + r]
            rows_tmp[buffer, pl.ds(r * 4, 4), :] = slots[pl.ds(slot * 4, 4), :]
        return [rows_tmp[buffer, pl.ds(j, 32, stride=4), :] for j in range(4)]

    other = 1 - core

    def core_copy(half, index):
        return pltpu.make_async_remote_copy(
            src_ref=core_send.at[half, index],
            dst_ref=core_recv.at[half, index],
            send_sem=core_sems.at[0, half, index],
            recv_sem=core_sems.at[1, half, index],
            device_id=device(core_=other),
            device_id_type=MESH,
        )

    @pl.loop(0, 16)
    def _(step):
        cells = gather(4 + step % 4, step // 4, other, step % 2)
        for j in range(4):
            core_send[1, j, step // 4, step % 4] = cells[j].astype(BF16)

    for k in range(4):
        core_copy(1, (y + 1 + k) % 4).start()
    for k in range(4):
        xk = (x + 1 + k) % 4

        @pl.loop(0, 4)
        def _(step):
            cells = gather(step, xk, other, step % 2)
            for j in range(4):
                core_send[0, xk, j, step] = cells[j].astype(BF16)

        core_copy(0, xk).start()

    def copy1(half, k):
        mine = y if half else x
        target = (mine + k) % 4
        return pltpu.make_async_remote_copy(
            src_ref=send1.at[half, target],
            dst_ref=recv1.at[half, mine],
            send_sem=sems1.at[0, half, k],
            recv_sem=sems1.at[1, half, k],
            device_id=device(y_=target) if half else device(x_=target),
            device_id_type=MESH,
        )

    for k in range(4):
        core_copy(1, (y + 1 + k) % 4).wait_recv()

    @pl.loop(0, 16)
    def _(step):
        cells = gather(4 + step % 4, step // 4, core, step % 2)
        for j in range(4):
            total = cells[j] + core_recv[1, j, step // 4, step % 4].astype(F32)
            send1[1, j, step // 4, step % 4] = total.astype(BF16)

    for k in (2, 1, 3):
        copy1(1, k).start()
    for k in (2, 1, 3, 0):
        xk = (x + k) % 4
        core_copy(0, xk).wait_recv()

        @pl.loop(0, 4)
        def _(step):
            cells = gather(step, xk, core, step % 2)
            for j in range(4):
                total = cells[j] + core_recv[0, xk, j, step].astype(F32)
                send1[0, xk, j, step] = total.astype(BF16)

        if k:
            copy1(0, k).start()

    def received1(half, k):
        mine = y if half else x
        source = (mine + 4 - k) % 4
        return pltpu.make_async_remote_copy(
            src_ref=send1.at[half, source],
            dst_ref=recv1.at[half, source],
            send_sem=sems1.at[0, half, k],
            recv_sem=sems1.at[1, half, k],
            device_id=device(y_=source) if half else device(x_=source),
            device_id_type=MESH,
        )

    def copy2(half, k):
        mine = x if half else y
        target = (mine + k) % 4
        return pltpu.make_async_remote_copy(
            src_ref=send2.at[half, target],
            dst_ref=recv2.at[half, mine],
            send_sem=sems2.at[0, half, k],
            recv_sem=sems2.at[1, half, k],
            device_id=device(x_=target) if half else device(y_=target),
            device_id_type=MESH,
        )

    def received2(half, k):
        mine = x if half else y
        source = (mine + 4 - k) % 4
        return pltpu.make_async_remote_copy(
            src_ref=send2.at[half, source],
            dst_ref=recv2.at[half, source],
            send_sem=sems2.at[0, half, k],
            recv_sem=sems2.at[1, half, k],
            device_id=device(x_=source) if half else device(y_=source),
            device_id_type=MESH,
        )

    for half in (1, 0):
        mine = y if half else x
        other_axis = x if half else y
        for k in (1, 3, 2):
            received1(half, k).wait_recv()
        for k in (2, 1, 3, 0):
            index = (other_axis + k) % 4
            for cell in range(4):
                total = send1[half, mine, index, cell].astype(F32)
                for s in range(1, 4):
                    total = total + recv1[half, (mine + s) % 4, index, cell].astype(F32)
                send2[half, index, cell] = total.astype(BF16)
            if k:
                copy2(half, k).start()

    z = z_hi * 8 + z_lo
    lane16 = lax.broadcasted_iota(jnp.int32, (16, 128), 1)
    for half in (1, 0):
        mine = x if half else y
        for k in (1, 3, 2):
            received2(half, k).wait_recv()
        for cell in range(4):
            total = send2[half, mine, cell].astype(F32)
            for s in range(1, 4):
                total = total + recv2[half, (mine + s) % 4, cell].astype(F32)
            top, bottom = total[0:16], total[16:32]
            send3[half * 4 + cell] = jnp.where(
                lane16 < 64, top, pltpu.roll(bottom, 64, 1)
            ).astype(BF16)
            send3[8 + half * 4 + cell] = jnp.where(
                lane16 < 64, pltpu.roll(top, 64, 1), bottom
            ).astype(BF16)

    def copy3(k):
        target = (z + k) % 16
        return pltpu.make_async_remote_copy(
            src_ref=send3.at[target],
            dst_ref=recv3.at[z],
            send_sem=sems3.at[0, k],
            recv_sem=sems3.at[1, k],
            device_id=device(z_lo_=target % 8, z_hi_=target // 8),
            device_id_type=MESH,
        )

    def received3(k):
        source = (z + 16 - k) % 16
        return pltpu.make_async_remote_copy(
            src_ref=send3.at[source],
            dst_ref=recv3.at[source],
            send_sem=sems3.at[0, k],
            recv_sem=sems3.at[1, k],
            device_id=device(z_lo_=source % 8, z_hi_=source // 8),
            device_id_type=MESH,
        )

    for k in (8, 7, 9, 6, 10, 5, 11, 4, 12, 3, 13, 2, 14, 1, 15):
        copy3(k).start()
    total = send3[z].astype(F32)
    for k in (1, 15, 2, 14, 3, 13, 4, 12, 5, 11, 6, 10, 7, 9, 8):
        received3(k).wait_recv()
        total = total + recv3[(z + 16 - k) % 16].astype(F32)
    out[pl.ds(0, 16), :] = total[:, 0:64]
    out[pl.ds(16, 16), :] = total[:, 64:128]

    pltpu.make_async_copy(
        staging.at[pl.ds(0, 63)], arrived.at[pl.ds(0, 63)], face_sems.at[0]
    ).wait()
    for half in range(2):
        for k in range(4):
            core_copy(half, k).wait_send()
        for k in range(1, 4):
            copy1(half, k).wait_send()
            copy2(half, k).wait_send()
    for k in range(1, 16):
        copy3(k).wait_send()


def local(surface_raw, area_normals, kernel_weights, block_map, band_observers, band_lags):
    smem = pl.BlockSpec(memory_space=pltpu.SMEM)
    vmem = pl.BlockSpec(memory_space=pltpu.VMEM)
    weights = kernel_weights.reshape(6, 2048, 128)
    dma = pltpu.SemaphoreType.DMA
    return pl.pallas_call(
        kernel,
        out_shape=jax.ShapeDtypeStruct((32, 64), F32),
        in_specs=[smem, smem, smem, vmem, vmem, pl.BlockSpec(memory_space=pl.ANY)],
        out_specs=vmem,
        scratch_shapes=[
            pltpu.VMEM((2, 1024, 128), F32),
            pltpu.VMEM((64, 32, 128), BF16),
            pltpu.VMEM((64, 32, 128), BF16),
            pltpu.VMEM((6, 2048, 128), BF16),
            pltpu.VMEM((768, 1024), BF16),
            pltpu.VMEM((9, 2048, 128), F32),
            pltpu.VMEM((8192, 128), F32),
            pltpu.VMEM((2, 128, 128), F32),
            pltpu.VMEM((16, 128), jnp.int32),
            pltpu.SMEM((16, 128), jnp.int32),
            pltpu.VMEM((2, 4, 4, 4, 32, 128), BF16),
            pltpu.VMEM((2, 4, 4, 4, 32, 128), BF16),
            pltpu.VMEM((2, 4, 4, 4, 32, 128), BF16),
            pltpu.VMEM((2, 4, 4, 4, 32, 128), BF16),
            pltpu.VMEM((2, 4, 4, 32, 128), BF16),
            pltpu.VMEM((2, 4, 4, 32, 128), BF16),
            pltpu.VMEM((16, 16, 128), BF16),
            pltpu.VMEM((16, 16, 128), BF16),
            dma,
            dma,
            dma((2,)),
            dma((2, 2, 4)),
            dma((2, 2, 4)),
            dma((2, 2, 4)),
            dma((2, 16)),
        ],
        compiler_params=pltpu.CompilerParams(collective_id=0, has_side_effects=True),
    )(block_map, band_observers, band_lags, surface_raw, area_normals, weights)


def solution(mesh):
    placed = (
        P(None, ("cfd", "ac"), None),
        P(None, ("cfd", "ac")),
        P(None, None, None, ("cfd", "ac")),
        P("ac", "cfd", None),
        P(),
        P(),
    )
    return jax.shard_map(
        local, mesh=mesh, in_specs=placed, out_specs=P("cfd", "ac"), check_vma=False
    )
```

```python
import functools

import jax
import jax.numpy as jnp
from jax import lax
from jax.experimental import pallas as pl
from jax.experimental.pallas import tpu as pltpu
from jax.sharding import PartitionSpec as P

MESH = pl.DeviceIdType.MESH
F32 = jnp.float32
BF16 = jnp.bfloat16

PITCH = 9


def kernel(
    block_map,
    band_observers,
    band_lags,
    surface,
    normals,
    weights_hbm,
    out,
    face_rows,
    staging,
    arrived,
    weights,
    pressure_sources,
    thickness_sources,
    product,
    slots,
    rows_tmp,
    table_v,
    table,
    core_send,
    core_recv,
    send1,
    recv1,
    send2,
    recv2,
    send3,
    recv3,
    weight_sem,
    table_sem,
    face_sems,
    core_sems,
    sems1,
    sems2,
    sems3,
):
    cfd = lax.axis_index("cfd")
    ac = lax.axis_index("ac")
    z_lo = cfd // 8
    x = (cfd // 2) % 4
    core = cfd % 2
    y = ac // 2
    z_hi = ac % 2
    z = z_hi * 8 + z_lo

    def device(z_lo_=z_lo, x_=x, core_=core, y_=y, z_hi_=z_hi):
        return ((z_lo_ * 4 + x_) * 2 + core_, y_ * 2 + z_hi_)

    weight_copy = pltpu.make_async_copy(weights_hbm, weights, weight_sem)
    weight_copy.start()

    barrier = pltpu.get_barrier_semaphore()

    @pl.loop(1, 64)
    def _(offset):
        pl.semaphore_signal(
            barrier, inc=1, device_id=((cfd + offset) % 64, ac), device_id_type=MESH
        )

    for k in range(1, 4):
        pl.semaphore_signal(
            barrier, inc=1, device_id=device(y_=(y + k) % 4), device_id_type=MESH
        )

    for k in range(8):
        pl.semaphore_signal(
            barrier, inc=1, device_id=device(z_lo_=k, z_hi_=1 - z_hi), device_id_type=MESH
        )

    columns = jnp.transpose(
        jnp.concatenate([normals[...].astype(F32), jnp.zeros((5, 128), F32)], axis=0)
    )
    n0, n1, n2 = columns[:, 0:1], columns[:, 1:2], columns[:, 2:3]
    for tile in range(8):
        lanes = pl.ds(tile * 128, 128)
        along = surface[2, :, lanes].astype(F32) * n0
        along = along + surface[3, :, lanes].astype(F32) * n1
        along = along + surface[4, :, lanes].astype(F32) * n2
        face_rows[1, pl.ds(tile, 128, stride=8), :] = surface[1, :, lanes].astype(F32) * along
        face_rows[0, pl.ds(tile, 128, stride=8), :] = surface[0, :, lanes].astype(F32)

    @pl.loop(0, 64, unroll=4)
    def _(d):
        first = block_map[0, 0, d] * 16
        for series in range(2):
            staging[series, d] = face_rows[series, pl.ds(first, 16), :].astype(BF16)

    pl.semaphore_wait(barrier, 74)

    def send_block(series, dest_z, k):
        dest = (dest_z * 4 + (x + k // 2) % 4) * 2 + (core + k) % 2
        pltpu.make_async_remote_copy(
            src_ref=staging.at[series, dest],
            dst_ref=arrived.at[series, cfd],
            send_sem=face_sems.at[0, series],
            recv_sem=face_sems.at[1, series],
            device_id=(dest, ac),
            device_id_type=MESH,
        ).start()

    for series in range(2):

        @pl.loop(0, 7)
        def _(step):
            dz = 7 - step
            for sign in (1, -1):
                dest_z = z_lo + sign * dz

                @pl.when((dest_z >= 0) & (dest_z < 8))
                def _():
                    for k in range(8):
                        send_block(series, dest_z, k)

        for k in range(1, 8):
            send_block(series, z_lo, k)
        arrived[series, cfd] = staging[series, cfd]

    observer = lax.broadcasted_iota(jnp.int32, (64, 128), 0) * 32 + (
        lax.broadcasted_iota(jnp.int32, (64, 128), 1) % 32
    )

    def find(band, found):
        start = 511 - band_lags[band]
        row = band * (128 * PITCH) + lax.div(start, 128)
        code = row * 128 + 127 - lax.rem(start, 128)
        for m in range(128):
            found = jnp.where(
                observer == band_observers[band, m], code + m * PITCH * 128, found
            )
        return found

    table_v[...] = lax.fori_loop(0, 16, find, jnp.zeros((64, 128), jnp.int32))
    table_copy = pltpu.make_async_copy(table_v, table, table_sem)
    table_copy.start()
    weight_copy.wait()
    table_copy.wait()

    def faces_arrived(series):
        pltpu.make_async_copy(
            arrived.at[series, pl.ds(0, 63)],
            staging.at[series, pl.ds(0, 63)],
            face_sems.at[1, series],
        ).wait()
        for part in range(8):
            tile = arrived[series, pl.ds(part * 8, 8)].astype(F32)
            face_rows[series, pl.ds(part * 128, 128), :] = tile.reshape(128, 128)

    lane = lax.broadcasted_iota(jnp.int32, (128, 128), 1)

    def differences(series):
        rolled = None
        step_rolled = None
        for tile in range(8):
            now = face_rows[series, pl.ds(tile, 128, stride=8), :]
            turned = pltpu.roll(now, 1, 1)
            before = jnp.where(lane == 0, now if tile == 0 else rolled, turned)
            rolled = turned
            step = (now - before).astype(BF16).astype(F32)
            step_turned = pltpu.roll(step, 1, 1)
            step_before = jnp.where(
                lane == 0, jnp.zeros_like(step) if tile == 0 else step_rolled, step_turned
            )
            step_rolled = step_turned
            yield (
                pl.ds(tile * 128, 128),
                [value.astype(BF16) for value in (now, before, step, step_before)],
            )

    faces_arrived(0)
    for lanes, (now, before, step, step_before) in differences(0):
        for row, value in enumerate((step, now, step_before, before)):
            pressure_sources[pl.ds(row * 128, 128), lanes] = value

    @pl.loop(0, 4)
    def _(n):
        lanes = pl.ds(pl.multiple_of(n * 256, 256), 256)
        for m in range(2):
            rows = pl.ds(m * 1024, 1024)
            left = jnp.concatenate([weights[kc, rows, :] for kc in (1, 2, 4, 5)], axis=1)
            both = jnp.dot(left, pressure_sources[:, lanes], preferred_element_type=F32)
            product[2 * n, rows, :] = both[:, 0:128]
            product[2 * n + 1, rows, :] = both[:, 128:256]

    faces_arrived(1)
    for lanes, (now, before, step, step_before) in differences(1):
        thickness_sources[pl.ds(0, 128), lanes] = step
        thickness_sources[pl.ds(128, 128), lanes] = step_before

    @pl.loop(0, 4)
    def _(n):
        lanes = pl.ds(pl.multiple_of(n * 256, 256), 256)
        for m in range(2):
            rows = pl.ds(m * 1024, 1024)
            left = jnp.concatenate([weights[kc, rows, :] for kc in (0, 3)], axis=1)
            both = jnp.dot(left, thickness_sources[:, lanes], preferred_element_type=F32)
            for side in range(2):
                slots[pl.ds(m * 1024 * PITCH + 2 * n + side, 1024, stride=PITCH), :] = (
                    product[2 * n + side, rows, :] + both[:, side * 128 : side * 128 + 128]
                )

    lane4 = lax.broadcasted_iota(jnp.int32, (4, 128), 1)
    lane16 = lax.broadcasted_iota(jnp.int32, (16, 128), 1)

    def gather(half, block_x, block_core):
        for n in range(4):
            first = (((z + 5 + 2 * n + half) % 8) * 4 + block_x) * 2 + block_core
            for r in range(32):
                code = table[first, r]
                row = lax.shift_right_logical(code, 7)
                turn = code & 127
                rows_tmp[n, pl.ds(r * 4, 4), :] = jnp.where(
                    lane4 < turn,
                    pltpu.roll(slots[pl.ds(row, 4), :], turn, 1),
                    pltpu.roll(slots[pl.ds(row + 1, 4), :], turn, 1),
                )
        for n in range(4):
            chunk = ((z + 5 + 2 * n + half) % 16) // 8
            for j in range(4):
                top = rows_tmp[n, pl.ds(j, 16, stride=4), :]
                bottom = rows_tmp[n, pl.ds(64 + j, 16, stride=4), :]
                yield (
                    (chunk, j, n),
                    jnp.where(lane16 < 64, top, pltpu.roll(bottom, 64, 1)),
                )
                yield (
                    (1 - chunk, j, n),
                    jnp.where(lane16 < 64, pltpu.roll(top, 64, 1), bottom),
                )

    other = 1 - core

    def core_copy(half, chunk):
        return pltpu.make_async_remote_copy(
            src_ref=core_send.at[half, chunk],
            dst_ref=core_recv.at[half, chunk],
            send_sem=core_sems.at[0, half, chunk],
            recv_sem=core_sems.at[1, half, chunk],
            device_id=device(core_=other),
            device_id_type=MESH,
        )

    def spot(half, chunk, xk, j, n):
        return (half, chunk, j, xk, n) if half else (half, chunk, xk, j, n)

    for half in (1, 0):

        @pl.loop(0, 4)
        def _(xk):
            for (chunk, j, n), tile in gather(half, xk, other):
                core_send[spot(half, chunk, xk, j, n)] = tile.astype(BF16)

        for chunk in range(2):
            core_copy(half, chunk).start()

    def copies(stage, half, chunk, k, arriving):
        along_y = half == (stage == 1)
        mine = y if along_y else x
        peer = (mine + (4 - k if arriving else k)) % 4
        source, landing, sems = (send1, recv1, sems1) if stage == 1 else (send2, recv2, sems2)
        return pltpu.make_async_remote_copy(
            src_ref=source.at[half, chunk, peer],
            dst_ref=landing.at[half, chunk, peer if arriving else mine],
            send_sem=sems.at[0, half, chunk, k],
            recv_sem=sems.at[1, half, chunk, k],
            device_id=device(y_=peer) if along_y else device(x_=peer),
            device_id_type=MESH,
        )

    for half in (1, 0):
        for chunk in range(2):
            core_copy(half, chunk).wait_recv()

        @pl.loop(0, 4)
        def _(xk):
            for (chunk, j, n), tile in gather(half, xk, core):
                at = spot(half, chunk, xk, j, n)
                send1[at] = (tile + core_recv[at].astype(F32)).astype(BF16)

        for chunk in range(2):
            for k in (2, 1, 3):
                copies(1, half, chunk, k, False).start()

    def second(half, chunk):
        mine, across = (y, x) if half else (x, y)
        for k in (1, 3, 2):
            copies(1, half, chunk, k, True).wait_recv()
        for k in (2, 1, 3, 0):
            index = (across + k) % 4
            for n in range(4):
                total = send1[half, chunk, mine, index, n].astype(F32)
                for s in range(1, 4):
                    total = total + recv1[half, chunk, (mine + s) % 4, index, n].astype(F32)
                send2[half, chunk, index, n] = total.astype(BF16)
            if k:
                copies(2, half, chunk, k, False).start()

    def copy3(i, arriving):
        dz = (5 + i) % 16
        peer = (z + (16 - dz if arriving else dz)) % 16
        return pltpu.make_async_remote_copy(
            src_ref=send3.at[i],
            dst_ref=recv3.at[i],
            send_sem=sems3.at[0, i],
            recv_sem=sems3.at[1, i],
            device_id=device(z_lo_=peer % 8, z_hi_=peer // 8),
            device_id_type=MESH,
        )

    def third(half, chunk):
        mine = x if half else y
        for k in (1, 3, 2):
            copies(2, half, chunk, k, True).wait_recv()
        for n in ((2, 1, 3, 0), (1, 2, 0, 3))[half]:
            total = send2[half, chunk, mine, n].astype(F32)
            for s in range(1, 4):
                total = total + recv2[half, chunk, (mine + s) % 4, n].astype(F32)
            i = chunk * 8 + 2 * n + half
            send3[i] = total.astype(BF16)
            if i != 11:
                copy3(i, False).start()

    for chunk in range(2):
        for half in (1, 0):
            second(half, chunk)
        for half in (1, 0):
            third(half, chunk)

    total = send3[11].astype(F32)
    for i in (10, 12, 9, 13, 8, 14, 15, 7, 0, 6, 1, 5, 2, 4, 3):
        copy3(i, True).wait_recv()
        total = total + recv3[i].astype(F32)
    out[pl.ds(0, 16), :] = total[:, 0:64]
    out[pl.ds(16, 16), :] = total[:, 64:128]

    for series in range(2):
        pltpu.make_async_copy(
            staging.at[series, pl.ds(0, 63)],
            arrived.at[series, pl.ds(0, 63)],
            face_sems.at[0, series],
        ).wait()
    for half in range(2):
        for chunk in range(2):
            core_copy(half, chunk).wait_send()
            for k in range(1, 4):
                copies(1, half, chunk, k, False).wait_send()
                copies(2, half, chunk, k, False).wait_send()
    for i in range(16):
        if i != 11:
            copy3(i, False).wait_send()


def local(surface_raw, area_normals, kernel_weights, block_map, band_observers, band_lags):
    smem = pl.BlockSpec(memory_space=pltpu.SMEM)
    vmem = pl.BlockSpec(memory_space=pltpu.VMEM)
    weights = kernel_weights.reshape(6, 2048, 128)
    dma = pltpu.SemaphoreType.DMA
    return pl.pallas_call(
        kernel,
        out_shape=jax.ShapeDtypeStruct((32, 64), F32),
        in_specs=[smem, smem, smem, vmem, vmem, pl.BlockSpec(memory_space=pl.ANY)],
        out_specs=vmem,
        scratch_shapes=[
            pltpu.VMEM((2, 1024, 128), F32),
            pltpu.VMEM((2, 64, 16, 128), BF16),
            pltpu.VMEM((2, 64, 16, 128), BF16),
            pltpu.VMEM((6, 2048, 128), BF16),
            pltpu.VMEM((512, 1024), BF16),
            pltpu.VMEM((256, 1024), BF16),
            pltpu.VMEM((8, 2048, 128), F32),
            pltpu.VMEM((2048 * PITCH, 128), F32),
            pltpu.VMEM((4, 128, 128), F32),
            pltpu.VMEM((64, 128), jnp.int32),
            pltpu.SMEM((64, 128), jnp.int32),
            pltpu.VMEM((2, 2, 4, 4, 4, 16, 128), BF16),
            pltpu.VMEM((2, 2, 4, 4, 4, 16, 128), BF16),
            pltpu.VMEM((2, 2, 4, 4, 4, 16, 128), BF16),
            pltpu.VMEM((2, 2, 4, 4, 4, 16, 128), BF16),
            pltpu.VMEM((2, 2, 4, 4, 16, 128), BF16),
            pltpu.VMEM((2, 2, 4, 4, 16, 128), BF16),
            pltpu.VMEM((16, 16, 128), BF16),
            pltpu.VMEM((16, 16, 128), BF16),
            dma,
            dma,
            dma((2, 2)),
            dma((2, 2, 2)),
            dma((2, 2, 2, 4)),
            dma((2, 2, 2, 4)),
            dma((2, 16)),
        ],
        compiler_params=pltpu.CompilerParams(collective_id=0, has_side_effects=True),
    )(block_map, band_observers, band_lags, surface_raw, area_normals, weights)


def solution(mesh):
    placed = (
        P(None, ("cfd", "ac"), None),
        P(None, ("cfd", "ac")),
        P(None, None, None, ("cfd", "ac")),
        P("ac", "cfd", None),
        P(),
        P(),
    )
    return jax.shard_map(
        local, mesh=mesh, in_specs=placed, out_specs=P("cfd", "ac"), check_vma=False
    )
```

```python
import functools

import jax
import jax.numpy as jnp
from jax import lax
from jax.experimental import pallas as pl
from jax.experimental.pallas import tpu as pltpu
from jax.sharding import PartitionSpec as P

MESH = pl.DeviceIdType.MESH
F32 = jnp.float32
BF16 = jnp.bfloat16

PITCH = 9


def kernel(
    block_map_hbm,
    band_observers_hbm,
    band_lags_hbm,
    surface_hbm,
    normals_hbm,
    weights_hbm,
    out,
    block_map,
    band_observers,
    band_lags,
    surface,
    normals,
    face_rows,
    staging,
    arrived,
    weights,
    pressure_sources,
    thickness_sources,
    product,
    slots,
    rows_tmp,
    table_v,
    table,
    core_send,
    core_recv,
    send1,
    recv1,
    send2,
    recv2,
    send3,
    recv3,
    round_sem,
    input_sems,
    table_sem,
    face_sems,
    core_sems,
    sems1,
    sems2,
    sems3,
):
    cfd = lax.axis_index("cfd")
    ac = lax.axis_index("ac")
    z_lo = cfd // 8
    x = (cfd // 2) % 4
    core = cfd % 2
    y = ac // 2
    z_hi = ac % 2
    z = z_hi * 8 + z_lo

    def device(z_lo_=z_lo, x_=x, core_=core, y_=y, z_hi_=z_hi):
        return ((z_lo_ * 4 + x_) * 2 + core_, y_ * 2 + z_hi_)

    barrier = pltpu.get_barrier_semaphore()

    for dz in (4, -4, 3, -3, 2, -2, 1, -1, 0):
        there = (z + 16 + dz) % 16
        for k in range(8):
            if dz or k:
                pl.semaphore_signal(
                    barrier,
                    inc=1,
                    device_id=device(
                        there % 8, (x + k // 2) % 4, (core + k) % 2, y, there // 8
                    ),
                    device_id_type=MESH,
                )
    for k in range(1, 4):
        pl.semaphore_signal(
            barrier, inc=1, device_id=device(y_=(y + k) % 4), device_id_type=MESH
        )

    inputs = [
        pltpu.make_async_copy(source, copy, input_sems.at[n])
        for n, (source, copy) in enumerate(
            (
                (surface_hbm, surface),
                (normals_hbm, normals),
                (block_map_hbm, block_map),
                (band_lags_hbm, band_lags),
                (band_observers_hbm, band_observers),
                (weights_hbm, weights),
            )
        )
    ]
    for copy in inputs:
        copy.start()
    for copy in inputs[:3]:
        copy.wait()

    columns = jnp.transpose(
        jnp.concatenate([normals[...].astype(F32), jnp.zeros((5, 128), F32)], axis=0)
    )
    n0, n1, n2 = columns[:, 0:1], columns[:, 1:2], columns[:, 2:3]
    for tile in range(8):
        lanes = pl.ds(tile * 128, 128)
        along = surface[2, :, lanes].astype(F32) * n0
        along = along + surface[3, :, lanes].astype(F32) * n1
        along = along + surface[4, :, lanes].astype(F32) * n2
        face_rows[1, pl.ds(tile, 128, stride=8), :] = surface[1, :, lanes].astype(F32) * along
        face_rows[0, pl.ds(tile, 128, stride=8), :] = surface[0, :, lanes].astype(F32)

    @pl.loop(0, 64, unroll=4)
    def _(d):
        first = block_map[0, 0, d] * 16
        for series in range(2):
            staging[series, d] = face_rows[series, pl.ds(first, 16), :].astype(BF16)

    pl.semaphore_wait(barrier, 74)
    for dz in (4, -4):
        there = (z + 16 + dz) % 16
        pl.semaphore_signal(
            round_sem,
            inc=1,
            device_id=device(z_lo_=there % 8, z_hi_=there // 8),
            device_id_type=MESH,
        )

    def send_block(series, dest_z, k):
        dest = (dest_z * 4 + (x + k // 2) % 4) * 2 + (core + k) % 2
        pltpu.make_async_remote_copy(
            src_ref=staging.at[series, dest],
            dst_ref=arrived.at[series, cfd],
            send_sem=face_sems.at[0, series],
            recv_sem=face_sems.at[1, series],
            device_id=(dest, ac),
            device_id_type=MESH,
        ).start()

    def send_far_to_near(series, farthest, nearest):
        @pl.loop(0, farthest - nearest + 1)
        def _(step):
            dz = farthest - step
            for sign in (1, -1):
                dest_z = z_lo + sign * dz

                @pl.when((dest_z >= 0) & (dest_z < 8))
                def _():
                    for k in range(8):
                        send_block(series, dest_z, k)

    send_far_to_near(0, 4, 1)
    pl.semaphore_wait(round_sem, 2)
    send_far_to_near(0, 7, 5)
    for k in range(1, 8):
        send_block(0, z_lo, k)
    send_far_to_near(1, 7, 1)
    for k in range(1, 8):
        send_block(1, z_lo, k)
    for series in range(2):
        arrived[series, cfd] = staging[series, cfd]

    for copy in inputs[3:]:
        copy.wait()

    observer = lax.broadcasted_iota(jnp.int32, (64, 128), 0) * 32 + (
        lax.broadcasted_iota(jnp.int32, (64, 128), 1) % 32
    )

    def find(band, found):
        start = 511 - band_lags[band]
        row = band * (128 * PITCH) + lax.div(start, 128)
        code = row * 128 + 127 - lax.rem(start, 128)
        for m in range(128):
            found = jnp.where(
                observer == band_observers[band, m], code + m * PITCH * 128, found
            )
        return found

    table_v[...] = lax.fori_loop(0, 16, find, jnp.zeros((64, 128), jnp.int32))
    table_copy = pltpu.make_async_copy(table_v, table, table_sem)
    table_copy.start()
    table_copy.wait()

    def faces_arrived(series):
        pltpu.make_async_copy(
            arrived.at[series, pl.ds(0, 63)],
            staging.at[series, pl.ds(0, 63)],
            face_sems.at[1, series],
        ).wait()
        for part in range(8):
            tile = arrived[series, pl.ds(part * 8, 8)].astype(F32)
            face_rows[series, pl.ds(part * 128, 128), :] = tile.reshape(128, 128)

    lane = lax.broadcasted_iota(jnp.int32, (128, 128), 1)

    def differences(series):
        rolled = None
        step_rolled = None
        for tile in range(8):
            now = face_rows[series, pl.ds(tile, 128, stride=8), :]
            turned = pltpu.roll(now, 1, 1)
            before = jnp.where(lane == 0, now if tile == 0 else rolled, turned)
            rolled = turned
            step = (now - before).astype(BF16).astype(F32)
            step_turned = pltpu.roll(step, 1, 1)
            step_before = jnp.where(
                lane == 0, jnp.zeros_like(step) if tile == 0 else step_rolled, step_turned
            )
            step_rolled = step_turned
            yield (
                pl.ds(tile * 128, 128),
                [value.astype(BF16) for value in (now, before, step, step_before)],
            )

    faces_arrived(0)
    for lanes, (now, before, step, step_before) in differences(0):
        for row, value in enumerate((step, now, step_before, before)):
            pressure_sources[pl.ds(row * 128, 128), lanes] = value

    @pl.loop(0, 4)
    def _(n):
        lanes = pl.ds(pl.multiple_of(n * 256, 256), 256)
        for m in range(2):
            rows = pl.ds(m * 1024, 1024)
            left = jnp.concatenate([weights[kc, rows, :] for kc in (1, 2, 4, 5)], axis=1)
            both = jnp.dot(left, pressure_sources[:, lanes], preferred_element_type=F32)
            product[2 * n, rows, :] = both[:, 0:128]
            product[2 * n + 1, rows, :] = both[:, 128:256]

    faces_arrived(1)
    for lanes, (now, before, step, step_before) in differences(1):
        thickness_sources[pl.ds(0, 128), lanes] = step
        thickness_sources[pl.ds(128, 128), lanes] = step_before

    @pl.loop(0, 4, unroll=4)
    def _(n):
        lanes = pl.ds(pl.multiple_of(n * 256, 256), 256)
        for m in range(2):
            rows = pl.ds(m * 1024, 1024)
            left = jnp.concatenate([weights[kc, rows, :] for kc in (0, 3)], axis=1)
            both = jnp.dot(left, thickness_sources[:, lanes], preferred_element_type=F32)
            for side in range(2):
                slots[pl.ds(m * 1024 * PITCH + 2 * n + side, 1024, stride=PITCH), :] = (
                    product[2 * n + side, rows, :] + both[:, side * 128 : side * 128 + 128]
                )

    back4 = 127 - lax.broadcasted_iota(jnp.int32, (4, 128), 1)
    lane16 = lax.broadcasted_iota(jnp.int32, (16, 128), 1)

    def gather(half, block_x, block_core):
        for n in range(5):
            if n < 4:
                first = (((z + 5 + 2 * n + half) % 8) * 4 + block_x) * 2 + block_core
                for r in range(32):
                    code = table[first, r]
                    row = lax.shift_right_logical(code, 7)
                    turn = code & 127
                    picked = jnp.where(
                        back4 < turn, slots[pl.ds(row, 4), :], slots[pl.ds(row + 1, 4), :]
                    )
                    rows_tmp[n, pl.ds(r * 4, 4), :] = pltpu.roll(picked, turn, 1)
            if n > 0:
                m = n - 1
                chunk = ((z + 5 + 2 * m + half) % 16) // 8
                for j in range(4):
                    top = rows_tmp[m, pl.ds(j, 16, stride=4), :]
                    bottom = rows_tmp[m, pl.ds(64 + j, 16, stride=4), :]
                    yield (
                        (chunk, j, m),
                        jnp.where(lane16 < 64, top, pltpu.roll(bottom, 64, 1)),
                    )
                    yield (
                        (1 - chunk, j, m),
                        jnp.where(lane16 < 64, pltpu.roll(top, 64, 1), bottom),
                    )

    other = 1 - core

    def core_copy(half, chunk):
        return pltpu.make_async_remote_copy(
            src_ref=core_send.at[half, chunk],
            dst_ref=core_recv.at[half, chunk],
            send_sem=core_sems.at[0, half, chunk],
            recv_sem=core_sems.at[1, half, chunk],
            device_id=device(core_=other),
            device_id_type=MESH,
        )

    def spot(half, chunk, xk, j, n):
        return (half, chunk, j, xk, n) if half else (half, chunk, xk, j, n)

    for half in (1, 0):

        @pl.loop(0, 4, unroll=2)
        def _(xk):
            for (chunk, j, n), tile in gather(half, xk, other):
                core_send[spot(half, chunk, xk, j, n)] = tile.astype(BF16)

        for chunk in range(2):
            core_copy(half, chunk).start()

    def copies(stage, half, chunk, k, arriving):
        along_y = half == (stage == 1)
        mine = y if along_y else x
        peer = (mine + (4 - k if arriving else k)) % 4
        source, landing, sems = (send1, recv1, sems1) if stage == 1 else (send2, recv2, sems2)
        return pltpu.make_async_remote_copy(
            src_ref=source.at[half, chunk, peer],
            dst_ref=landing.at[half, chunk, peer if arriving else mine],
            send_sem=sems.at[0, half, chunk, k],
            recv_sem=sems.at[1, half, chunk, k],
            device_id=device(y_=peer) if along_y else device(x_=peer),
            device_id_type=MESH,
        )

    for half in (1, 0):
        for chunk in range(2):
            core_copy(half, chunk).wait_recv()

        @pl.loop(0, 4, unroll=2)
        def _(xk):
            for (chunk, j, n), tile in gather(half, xk, core):
                at = spot(half, chunk, xk, j, n)
                send1[at] = (tile + core_recv[at].astype(F32)).astype(BF16)

        for chunk in range(2):
            for k in (2, 1, 3):
                copies(1, half, chunk, k, False).start()

    def second(half, chunk):
        mine, across = (y, x) if half else (x, y)
        for k in (1, 3, 2):
            copies(1, half, chunk, k, True).wait_recv()
        for k in (2, 1, 3, 0):
            index = (across + k) % 4
            for n in range(4):
                total = send1[half, chunk, mine, index, n].astype(F32)
                for s in range(1, 4):
                    total = total + recv1[half, chunk, (mine + s) % 4, index, n].astype(F32)
                send2[half, chunk, index, n] = total.astype(BF16)
            if k:
                copies(2, half, chunk, k, False).start()

    def copy3(i, arriving):
        dz = (5 + i) % 16
        peer = (z + (16 - dz if arriving else dz)) % 16
        return pltpu.make_async_remote_copy(
            src_ref=send3.at[i],
            dst_ref=recv3.at[i],
            send_sem=sems3.at[0, i],
            recv_sem=sems3.at[1, i],
            device_id=device(z_lo_=peer % 8, z_hi_=peer // 8),
            device_id_type=MESH,
        )

    def third(half, chunk):
        mine = x if half else y
        for k in (1, 3, 2):
            copies(2, half, chunk, k, True).wait_recv()
        for n in ((2, 1, 3, 0), (1, 2, 0, 3))[half]:
            total = send2[half, chunk, mine, n].astype(F32)
            for s in range(1, 4):
                total = total + recv2[half, chunk, (mine + s) % 4, n].astype(F32)
            i = chunk * 8 + 2 * n + half
            send3[i] = total.astype(BF16)
            if i != 11:
                copy3(i, False).start()

    for chunk in range(2):
        for half in (1, 0):
            second(half, chunk)
        for half in (1, 0):
            third(half, chunk)

    total = send3[11].astype(F32)
    for i in (10, 12, 9, 13, 8, 14, 15, 7, 0, 6, 1, 5, 2, 4, 3):
        copy3(i, True).wait_recv()
        total = total + recv3[i].astype(F32)
    out[pl.ds(0, 16), :] = total[:, 0:64]
    out[pl.ds(16, 16), :] = total[:, 64:128]

    for series in range(2):
        pltpu.make_async_copy(
            staging.at[series, pl.ds(0, 63)],
            arrived.at[series, pl.ds(0, 63)],
            face_sems.at[0, series],
        ).wait()
    for half in range(2):
        for chunk in range(2):
            core_copy(half, chunk).wait_send()
            for k in range(1, 4):
                copies(1, half, chunk, k, False).wait_send()
                copies(2, half, chunk, k, False).wait_send()
    for i in range(16):
        if i != 11:
            copy3(i, False).wait_send()


def local(surface_raw, area_normals, kernel_weights, block_map, band_observers, band_lags):
    anywhere = pl.BlockSpec(memory_space=pl.ANY)
    weights = kernel_weights.reshape(6, 2048, 128)
    dma = pltpu.SemaphoreType.DMA
    return pl.pallas_call(
        kernel,
        out_shape=jax.ShapeDtypeStruct((32, 64), F32),
        in_specs=[anywhere] * 6,
        out_specs=pl.BlockSpec(memory_space=pltpu.VMEM),
        scratch_shapes=[
            pltpu.SMEM((1, 1, 64), jnp.int32),
            pltpu.SMEM((16, 128), jnp.int32),
            pltpu.SMEM((16,), jnp.int32),
            pltpu.VMEM((5, 128, 1024), BF16),
            pltpu.VMEM((3, 128), BF16),
            pltpu.VMEM((2, 1024, 128), F32),
            pltpu.VMEM((2, 64, 16, 128), BF16),
            pltpu.VMEM((2, 64, 16, 128), BF16),
            pltpu.VMEM((6, 2048, 128), BF16),
            pltpu.VMEM((512, 1024), BF16),
            pltpu.VMEM((256, 1024), BF16),
            pltpu.VMEM((8, 2048, 128), F32),
            pltpu.VMEM((2048 * PITCH, 128), F32),
            pltpu.VMEM((4, 128, 128), F32),
            pltpu.VMEM((64, 128), jnp.int32),
            pltpu.SMEM((64, 128), jnp.int32),
            pltpu.VMEM((2, 2, 4, 4, 4, 16, 128), BF16),
            pltpu.VMEM((2, 2, 4, 4, 4, 16, 128), BF16),
            pltpu.VMEM((2, 2, 4, 4, 4, 16, 128), BF16),
            pltpu.VMEM((2, 2, 4, 4, 4, 16, 128), BF16),
            pltpu.VMEM((2, 2, 4, 4, 16, 128), BF16),
            pltpu.VMEM((2, 2, 4, 4, 16, 128), BF16),
            pltpu.VMEM((16, 16, 128), BF16),
            pltpu.VMEM((16, 16, 128), BF16),
            pltpu.SemaphoreType.REGULAR,
            dma((6,)),
            dma,
            dma((2, 2)),
            dma((2, 2, 2)),
            dma((2, 2, 2, 4)),
            dma((2, 2, 2, 4)),
            dma((2, 16)),
        ],
        compiler_params=pltpu.CompilerParams(collective_id=0, has_side_effects=True),
    )(block_map, band_observers, band_lags, surface_raw, area_normals, weights)


def solution(mesh):
    placed = (
        P(None, ("cfd", "ac"), None),
        P(None, ("cfd", "ac")),
        P(None, None, None, ("cfd", "ac")),
        P("ac", "cfd", None),
        P(),
        P(),
    )
    return jax.shard_map(
        local, mesh=mesh, in_specs=placed, out_specs=P("cfd", "ac"), check_vma=False
    )
```

```python
import functools

import jax
import jax.numpy as jnp
from jax import lax
from jax.experimental import pallas as pl
from jax.experimental.pallas import tpu as pltpu
from jax.sharding import PartitionSpec as P

MESH = pl.DeviceIdType.MESH
F32 = jnp.float32
BF16 = jnp.bfloat16

PITCH = 9


def kernel(
    block_map_hbm,
    band_observers_hbm,
    band_lags_hbm,
    surface_hbm,
    normals_hbm,
    weights_hbm,
    out,
    block_map,
    band_observers,
    band_lags,
    surface,
    normals,
    face_rows,
    staging,
    arrived,
    weights,
    pressure_sources,
    thickness_sources,
    product,
    slots,
    rows_tmp,
    table_v,
    table,
    core_send,
    core_recv,
    send1,
    recv1,
    send2,
    recv2,
    send3,
    recv3,
    round_sems,
    input_sems,
    table_sem,
    face_sems,
    core_sems,
    sems1,
    sems2,
    sems3,
):
    cfd = lax.axis_index("cfd")
    ac = lax.axis_index("ac")
    z_lo = cfd // 8
    x = (cfd // 2) % 4
    core = cfd % 2
    y = ac // 2
    z_hi = ac % 2
    z = z_hi * 8 + z_lo

    def device(z_lo_=z_lo, x_=x, core_=core, y_=y, z_hi_=z_hi):
        return ((z_lo_ * 4 + x_) * 2 + core_, y_ * 2 + z_hi_)

    barrier = pltpu.get_barrier_semaphore()

    for dz in (2, -2, 1, -1, 0):
        there = (z + 16 + dz) % 16
        for k in range(8):
            if dz or k:
                pl.semaphore_signal(
                    barrier,
                    inc=1,
                    device_id=device(
                        there % 8, (x + k // 2) % 4, (core + k) % 2, y, there // 8
                    ),
                    device_id_type=MESH,
                )
    for k in range(1, 4):
        pl.semaphore_signal(
            barrier, inc=1, device_id=device(y_=(y + k) % 4), device_id_type=MESH
        )

    inputs = [
        pltpu.make_async_copy(source, copy, input_sems.at[n])
        for n, (source, copy) in enumerate(
            (
                (surface_hbm, surface),
                (normals_hbm, normals),
                (block_map_hbm, block_map),
                (band_lags_hbm, band_lags),
                (band_observers_hbm, band_observers),
                (weights_hbm, weights),
            )
        )
    ]
    for copy in inputs:
        copy.start()
    for copy in inputs[:3]:
        copy.wait()

    columns = jnp.transpose(
        jnp.concatenate([normals[...].astype(F32), jnp.zeros((5, 128), F32)], axis=0)
    )
    n0, n1, n2 = columns[:, 0:1], columns[:, 1:2], columns[:, 2:3]
    for tile in range(8):
        lanes = pl.ds(tile * 128, 128)
        along = surface[2, :, lanes].astype(F32) * n0
        along = along + surface[3, :, lanes].astype(F32) * n1
        along = along + surface[4, :, lanes].astype(F32) * n2
        face_rows[1, pl.ds(tile, 128, stride=8), :] = surface[1, :, lanes].astype(F32) * along
        face_rows[0, pl.ds(tile, 128, stride=8), :] = surface[0, :, lanes].astype(F32)

    @pl.loop(0, 64, unroll=4)
    def _(d):
        first = block_map[0, 0, d] * 16
        for series in range(2):
            staging[series, d] = face_rows[series, pl.ds(first, 16), :].astype(BF16)

    pl.semaphore_wait(barrier, 42)
    def tell(step):
        for dz in (2, -2):
            there = (z + 16 + dz) % 16
            pl.semaphore_signal(
                round_sems.at[step],
                inc=1,
                device_id=device(z_lo_=there % 8, z_hi_=there // 8),
                device_id_type=MESH,
            )

    tell(0)

    def send_block(series, dest_z, k):
        dest = (dest_z * 4 + (x + k // 2) % 4) * 2 + (core + k) % 2
        pltpu.make_async_remote_copy(
            src_ref=staging.at[series, dest],
            dst_ref=arrived.at[series, cfd],
            send_sem=face_sems.at[0, series],
            recv_sem=face_sems.at[1, series],
            device_id=(dest, ac),
            device_id_type=MESH,
        ).start()

    def send_far_to_near(series, farthest, nearest):
        @pl.loop(0, farthest - nearest + 1)
        def _(step):
            dz = farthest - step
            for sign in (1, -1):
                dest_z = z_lo + sign * dz

                @pl.when((dest_z >= 0) & (dest_z < 8))
                def _():
                    for k in range(8):
                        send_block(series, dest_z, k)

    send_far_to_near(0, 2, 1)
    for k in range(1, 8):
        send_block(0, z_lo, k)
    pl.semaphore_wait(round_sems.at[0], 2)
    tell(1)
    send_far_to_near(0, 4, 3)
    pl.semaphore_wait(round_sems.at[1], 2)
    tell(2)
    send_far_to_near(0, 6, 5)
    pl.semaphore_wait(round_sems.at[2], 2)
    send_far_to_near(0, 7, 7)
    send_far_to_near(1, 7, 1)
    for k in range(1, 8):
        send_block(1, z_lo, k)
    for series in range(2):
        arrived[series, cfd] = staging[series, cfd]

    for copy in inputs[3:]:
        copy.wait()

    observer = lax.broadcasted_iota(jnp.int32, (64, 128), 0) * 32 + (
        lax.broadcasted_iota(jnp.int32, (64, 128), 1) % 32
    )

    def find(band, found):
        start = 511 - band_lags[band]
        row = band * (128 * PITCH) + lax.div(start, 128)
        code = row * 128 + 127 - lax.rem(start, 128)
        for m in range(128):
            found = jnp.where(
                observer == band_observers[band, m], code + m * PITCH * 128, found
            )
        return found

    table_v[...] = lax.fori_loop(0, 16, find, jnp.zeros((64, 128), jnp.int32))
    table_copy = pltpu.make_async_copy(table_v, table, table_sem)
    table_copy.start()
    table_copy.wait()

    def faces_arrived(series):
        pltpu.make_async_copy(
            arrived.at[series, pl.ds(0, 63)],
            staging.at[series, pl.ds(0, 63)],
            face_sems.at[1, series],
        ).wait()
        for part in range(8):
            tile = arrived[series, pl.ds(part * 8, 8)].astype(F32)
            face_rows[series, pl.ds(part * 128, 128), :] = tile.reshape(128, 128)

    lane = lax.broadcasted_iota(jnp.int32, (128, 128), 1)

    def differences(series):
        rolled = None
        step_rolled = None
        for tile in range(8):
            now = face_rows[series, pl.ds(tile, 128, stride=8), :]
            turned = pltpu.roll(now, 1, 1)
            before = jnp.where(lane == 0, now if tile == 0 else rolled, turned)
            rolled = turned
            step = (now - before).astype(BF16).astype(F32)
            step_turned = pltpu.roll(step, 1, 1)
            step_before = jnp.where(
                lane == 0, jnp.zeros_like(step) if tile == 0 else step_rolled, step_turned
            )
            step_rolled = step_turned
            yield (
                pl.ds(tile * 128, 128),
                [value.astype(BF16) for value in (now, before, step, step_before)],
            )

    faces_arrived(0)
    for lanes, (now, before, step, step_before) in differences(0):
        for row, value in enumerate((step, now, step_before, before)):
            pressure_sources[pl.ds(row * 128, 128), lanes] = value

    @pl.loop(0, 4)
    def _(n):
        lanes = pl.ds(pl.multiple_of(n * 256, 256), 256)
        for m in range(2):
            rows = pl.ds(m * 1024, 1024)
            left = jnp.concatenate([weights[kc, rows, :] for kc in (1, 2, 4, 5)], axis=1)
            both = jnp.dot(left, pressure_sources[:, lanes], preferred_element_type=F32)
            product[2 * n, rows, :] = both[:, 0:128]
            product[2 * n + 1, rows, :] = both[:, 128:256]

    faces_arrived(1)
    for lanes, (now, before, step, step_before) in differences(1):
        thickness_sources[pl.ds(0, 128), lanes] = step
        thickness_sources[pl.ds(128, 128), lanes] = step_before

    @pl.loop(0, 4, unroll=4)
    def _(n):
        lanes = pl.ds(pl.multiple_of(n * 256, 256), 256)
        for m in range(2):
            rows = pl.ds(m * 1024, 1024)
            left = jnp.concatenate([weights[kc, rows, :] for kc in (0, 3)], axis=1)
            both = jnp.dot(left, thickness_sources[:, lanes], preferred_element_type=F32)
            for side in range(2):
                slots[pl.ds(m * 1024 * PITCH + 2 * n + side, 1024, stride=PITCH), :] = (
                    product[2 * n + side, rows, :] + both[:, side * 128 : side * 128 + 128]
                )

    back4 = 127 - lax.broadcasted_iota(jnp.int32, (4, 128), 1)
    lane16 = lax.broadcasted_iota(jnp.int32, (16, 128), 1)

    def gather(half, block_x, block_core):
        for n in range(5):
            if n < 4:
                first = (((z + 5 + 2 * n + half) % 8) * 4 + block_x) * 2 + block_core
                for r in range(32):
                    code = table[first, r]
                    row = lax.shift_right_logical(code, 7)
                    turn = code & 127
                    picked = jnp.where(
                        back4 < turn, slots[pl.ds(row, 4), :], slots[pl.ds(row + 1, 4), :]
                    )
                    rows_tmp[n, pl.ds(r * 4, 4), :] = pltpu.roll(picked, turn, 1)
            if n > 0:
                m = n - 1
                chunk = ((z + 5 + 2 * m + half) % 16) // 8
                for j in range(4):
                    top = rows_tmp[m, pl.ds(j, 16, stride=4), :]
                    bottom = rows_tmp[m, pl.ds(64 + j, 16, stride=4), :]
                    yield (
                        (chunk, j, m),
                        jnp.where(lane16 < 64, top, pltpu.roll(bottom, 64, 1)),
                    )
                    yield (
                        (1 - chunk, j, m),
                        jnp.where(lane16 < 64, pltpu.roll(top, 64, 1), bottom),
                    )

    other = 1 - core

    def core_copy(half, chunk):
        return pltpu.make_async_remote_copy(
            src_ref=core_send.at[half, chunk],
            dst_ref=core_recv.at[half, chunk],
            send_sem=core_sems.at[0, half, chunk],
            recv_sem=core_sems.at[1, half, chunk],
            device_id=device(core_=other),
            device_id_type=MESH,
        )

    def spot(half, chunk, xk, j, n):
        return (half, chunk, j, xk, n) if half else (half, chunk, xk, j, n)

    for half in (1, 0):

        @pl.loop(0, 4, unroll=2)
        def _(xk):
            for (chunk, j, n), tile in gather(half, xk, other):
                core_send[spot(half, chunk, xk, j, n)] = tile.astype(BF16)

        for chunk in range(2):
            core_copy(half, chunk).start()

    def copies(stage, half, chunk, k, arriving):
        along_y = half == (stage == 1)
        mine = y if along_y else x
        peer = (mine + (4 - k if arriving else k)) % 4
        source, landing, sems = (send1, recv1, sems1) if stage == 1 else (send2, recv2, sems2)
        return pltpu.make_async_remote_copy(
            src_ref=source.at[half, chunk, peer],
            dst_ref=landing.at[half, chunk, peer if arriving else mine],
            send_sem=sems.at[0, half, chunk, k],
            recv_sem=sems.at[1, half, chunk, k],
            device_id=device(y_=peer) if along_y else device(x_=peer),
            device_id_type=MESH,
        )

    for half in (1, 0):
        for chunk in range(2):
            core_copy(half, chunk).wait_recv()

        @pl.loop(0, 4, unroll=2)
        def _(xk):
            for (chunk, j, n), tile in gather(half, xk, core):
                at = spot(half, chunk, xk, j, n)
                send1[at] = (tile + core_recv[at].astype(F32)).astype(BF16)

        for chunk in range(2):
            for k in (2, 1, 3):
                copies(1, half, chunk, k, False).start()

    def second(half, chunk):
        mine, across = (y, x) if half else (x, y)
        for k in (1, 3, 2):
            copies(1, half, chunk, k, True).wait_recv()
        for k in (2, 1, 3, 0):
            index = (across + k) % 4
            for n in range(4):
                total = send1[half, chunk, mine, index, n].astype(F32)
                for s in range(1, 4):
                    total = total + recv1[half, chunk, (mine + s) % 4, index, n].astype(F32)
                send2[half, chunk, index, n] = total.astype(BF16)
            if k:
                copies(2, half, chunk, k, False).start()

    def copy3(i, arriving):
        dz = (5 + i) % 16
        peer = (z + (16 - dz if arriving else dz)) % 16
        return pltpu.make_async_remote_copy(
            src_ref=send3.at[i],
            dst_ref=recv3.at[i],
            send_sem=sems3.at[0, i],
            recv_sem=sems3.at[1, i],
            device_id=device(z_lo_=peer % 8, z_hi_=peer // 8),
            device_id_type=MESH,
        )

    def third(half, chunk):
        mine = x if half else y
        for k in (1, 3, 2):
            copies(2, half, chunk, k, True).wait_recv()
        for n in ((2, 1, 3, 0), (1, 2, 0, 3))[half]:
            total = send2[half, chunk, mine, n].astype(F32)
            for s in range(1, 4):
                total = total + recv2[half, chunk, (mine + s) % 4, n].astype(F32)
            i = chunk * 8 + 2 * n + half
            send3[i] = total.astype(BF16)
            if i != 11:
                copy3(i, False).start()

    for stage in (second, third):
        for chunk in range(2):
            for half in (1, 0):
                stage(half, chunk)

    total = send3[11].astype(F32)
    for i in (10, 12, 9, 13, 8, 14, 15, 7, 0, 6, 1, 5, 2, 4, 3):
        copy3(i, True).wait_recv()
        total = total + recv3[i].astype(F32)
    out[pl.ds(0, 16), :] = total[:, 0:64]
    out[pl.ds(16, 16), :] = total[:, 64:128]

    for series in range(2):
        pltpu.make_async_copy(
            staging.at[series, pl.ds(0, 63)],
            arrived.at[series, pl.ds(0, 63)],
            face_sems.at[0, series],
        ).wait()
    for half in range(2):
        for chunk in range(2):
            core_copy(half, chunk).wait_send()
            for k in range(1, 4):
                copies(1, half, chunk, k, False).wait_send()
                copies(2, half, chunk, k, False).wait_send()
    for i in range(16):
        if i != 11:
            copy3(i, False).wait_send()


def local(surface_raw, area_normals, kernel_weights, block_map, band_observers, band_lags):
    anywhere = pl.BlockSpec(memory_space=pl.ANY)
    weights = kernel_weights.reshape(6, 2048, 128)
    dma = pltpu.SemaphoreType.DMA
    return pl.pallas_call(
        kernel,
        out_shape=jax.ShapeDtypeStruct((32, 64), F32),
        in_specs=[anywhere] * 6,
        out_specs=pl.BlockSpec(memory_space=pltpu.VMEM),
        scratch_shapes=[
            pltpu.SMEM((1, 1, 64), jnp.int32),
            pltpu.SMEM((16, 128), jnp.int32),
            pltpu.SMEM((16,), jnp.int32),
            pltpu.VMEM((5, 128, 1024), BF16),
            pltpu.VMEM((3, 128), BF16),
            pltpu.VMEM((2, 1024, 128), F32),
            pltpu.VMEM((2, 64, 16, 128), BF16),
            pltpu.VMEM((2, 64, 16, 128), BF16),
            pltpu.VMEM((6, 2048, 128), BF16),
            pltpu.VMEM((512, 1024), BF16),
            pltpu.VMEM((256, 1024), BF16),
            pltpu.VMEM((8, 2048, 128), F32),
            pltpu.VMEM((2048 * PITCH, 128), F32),
            pltpu.VMEM((4, 128, 128), F32),
            pltpu.VMEM((64, 128), jnp.int32),
            pltpu.SMEM((64, 128), jnp.int32),
            pltpu.VMEM((2, 2, 4, 4, 4, 16, 128), BF16),
            pltpu.VMEM((2, 2, 4, 4, 4, 16, 128), BF16),
            pltpu.VMEM((2, 2, 4, 4, 4, 16, 128), BF16),
            pltpu.VMEM((2, 2, 4, 4, 4, 16, 128), BF16),
            pltpu.VMEM((2, 2, 4, 4, 16, 128), BF16),
            pltpu.VMEM((2, 2, 4, 4, 16, 128), BF16),
            pltpu.VMEM((16, 16, 128), BF16),
            pltpu.VMEM((16, 16, 128), BF16),
            pltpu.SemaphoreType.REGULAR((3,)),
            dma((6,)),
            dma,
            dma((2, 2)),
            dma((2, 2, 2)),
            dma((2, 2, 2, 4)),
            dma((2, 2, 2, 4)),
            dma((2, 16)),
        ],
        compiler_params=pltpu.CompilerParams(collective_id=0, has_side_effects=True),
    )(block_map, band_observers, band_lags, surface_raw, area_normals, weights)


def solution(mesh):
    placed = (
        P(None, ("cfd", "ac"), None),
        P(None, ("cfd", "ac")),
        P(None, None, None, ("cfd", "ac")),
        P("ac", "cfd", None),
        P(),
        P(),
    )
    return jax.shard_map(
        local, mesh=mesh, in_specs=placed, out_specs=P("cfd", "ac"), check_vma=False
    )
```

```python
import functools

import jax
import jax.numpy as jnp
from jax import lax
from jax.experimental import pallas as pl
from jax.experimental.pallas import tpu as pltpu
from jax.sharding import PartitionSpec as P

MESH = pl.DeviceIdType.MESH
F32 = jnp.float32
BF16 = jnp.bfloat16

PITCH = 9


def kernel(
    block_map_hbm,
    band_observers_hbm,
    band_lags_hbm,
    surface_hbm,
    normals_hbm,
    weights_hbm,
    out,
    block_map,
    band_observers,
    band_lags,
    surface,
    normals,
    face_rows,
    staging,
    arrived,
    weights,
    pressure_sources,
    thickness_sources,
    product,
    slots,
    rows_tmp,
    table_v,
    table,
    core_send,
    core_recv,
    send1,
    recv1,
    send2,
    recv2,
    send3,
    recv3,
    round_sems,
    input_sems,
    table_sem,
    face_sems,
    core_sems,
    sems1,
    sems2,
    sems3,
):
    cfd = lax.axis_index("cfd")
    ac = lax.axis_index("ac")
    z_lo = cfd // 8
    x = (cfd // 2) % 4
    core = cfd % 2
    y = ac // 2
    z_hi = ac % 2
    z = z_hi * 8 + z_lo

    def device(z_lo_=z_lo, x_=x, core_=core, y_=y, z_hi_=z_hi):
        return ((z_lo_ * 4 + x_) * 2 + core_, y_ * 2 + z_hi_)

    barrier = pltpu.get_barrier_semaphore()

    for dz in (2, -2, 1, -1, 0):
        there = (z + 16 + dz) % 16
        for k in range(8):
            if dz or k:
                pl.semaphore_signal(
                    barrier,
                    inc=1,
                    device_id=device(
                        there % 8, (x + k // 2) % 4, (core + k) % 2, y, there // 8
                    ),
                    device_id_type=MESH,
                )
    for k in range(1, 4):
        pl.semaphore_signal(
            barrier, inc=1, device_id=device(y_=(y + k) % 4), device_id_type=MESH
        )

    inputs = [
        pltpu.make_async_copy(source, copy, input_sems.at[n])
        for n, (source, copy) in enumerate(
            (
                (surface_hbm, surface),
                (normals_hbm, normals),
                (block_map_hbm, block_map),
                (band_lags_hbm, band_lags),
                (band_observers_hbm, band_observers),
                (weights_hbm, weights),
            )
        )
    ]
    for copy in inputs:
        copy.start()
    for copy in inputs[:3]:
        copy.wait()

    columns = jnp.transpose(
        jnp.concatenate([normals[...].astype(F32), jnp.zeros((5, 128), F32)], axis=0)
    )
    n0, n1, n2 = columns[:, 0:1], columns[:, 1:2], columns[:, 2:3]
    for tile in range(8):
        lanes = pl.ds(tile * 128, 128)
        along = surface[2, :, lanes].astype(F32) * n0
        along = along + surface[3, :, lanes].astype(F32) * n1
        along = along + surface[4, :, lanes].astype(F32) * n2
        face_rows[1, pl.ds(tile, 128, stride=8), :] = surface[1, :, lanes].astype(F32) * along
        face_rows[0, pl.ds(tile, 128, stride=8), :] = surface[0, :, lanes].astype(F32)

    @pl.loop(0, 64, unroll=4)
    def _(d):
        first = block_map[0, 0, d] * 16
        for series in range(2):
            staging[series, d] = face_rows[series, pl.ds(first, 16), :].astype(BF16)

    pl.semaphore_wait(barrier, 42)
    def tell(step):
        for dz in (2, -2):
            there = (z + 16 + dz) % 16
            pl.semaphore_signal(
                round_sems.at[step],
                inc=1,
                device_id=device(z_lo_=there % 8, z_hi_=there // 8),
                device_id_type=MESH,
            )

    tell(0)

    def send_block(series, dest_z, k):
        dest = (dest_z * 4 + (x + k // 2) % 4) * 2 + (core + k) % 2
        pltpu.make_async_remote_copy(
            src_ref=staging.at[series, dest],
            dst_ref=arrived.at[series, cfd],
            send_sem=face_sems.at[0, series],
            recv_sem=face_sems.at[1, series],
            device_id=(dest, ac),
            device_id_type=MESH,
        ).start()

    def send_far_to_near(series, farthest, nearest):
        @pl.loop(0, farthest - nearest + 1)
        def _(step):
            dz = farthest - step
            for sign in (1, -1):
                dest_z = z_lo + sign * dz

                @pl.when((dest_z >= 0) & (dest_z < 8))
                def _():
                    for k in range(8):
                        send_block(series, dest_z, k)

    send_far_to_near(0, 2, 1)
    for k in range(1, 8):
        send_block(0, z_lo, k)
    pl.semaphore_wait(round_sems.at[0], 2)
    tell(1)
    send_far_to_near(0, 4, 3)
    pl.semaphore_wait(round_sems.at[1], 2)
    tell(2)
    send_far_to_near(0, 6, 5)
    pl.semaphore_wait(round_sems.at[2], 2)
    send_far_to_near(0, 7, 7)
    send_far_to_near(1, 7, 1)
    for k in range(1, 8):
        send_block(1, z_lo, k)
    for series in range(2):
        arrived[series, cfd] = staging[series, cfd]

    for copy in inputs[3:]:
        copy.wait()

    observer = lax.broadcasted_iota(jnp.int32, (64, 128), 0) * 32 + (
        lax.broadcasted_iota(jnp.int32, (64, 128), 1) % 32
    )

    def find(band, found):
        start = 511 - band_lags[band]
        row = band * (128 * PITCH) + lax.div(start, 128)
        code = row * 128 + 127 - lax.rem(start, 128)
        for m in range(128):
            found = jnp.where(
                observer == band_observers[band, m], code + m * PITCH * 128, found
            )
        return found

    table_v[...] = lax.fori_loop(0, 16, find, jnp.zeros((64, 128), jnp.int32))
    table_copy = pltpu.make_async_copy(table_v, table, table_sem)
    table_copy.start()
    table_copy.wait()

    def faces_arrived(series):
        pltpu.make_async_copy(
            arrived.at[series, pl.ds(0, 63)],
            staging.at[series, pl.ds(0, 63)],
            face_sems.at[1, series],
        ).wait()
        for part in range(8):
            tile = arrived[series, pl.ds(part * 8, 8)].astype(F32)
            face_rows[series, pl.ds(part * 128, 128), :] = tile.reshape(128, 128)

    lane = lax.broadcasted_iota(jnp.int32, (128, 128), 1)

    def differences(series):
        rolled = None
        step_rolled = None
        for tile in range(8):
            now = face_rows[series, pl.ds(tile, 128, stride=8), :]
            turned = pltpu.roll(now, 1, 1)
            before = jnp.where(lane == 0, now if tile == 0 else rolled, turned)
            rolled = turned
            step = (now - before).astype(BF16).astype(F32)
            step_turned = pltpu.roll(step, 1, 1)
            step_before = jnp.where(
                lane == 0, jnp.zeros_like(step) if tile == 0 else step_rolled, step_turned
            )
            step_rolled = step_turned
            yield (
                pl.ds(tile * 128, 128),
                [value.astype(BF16) for value in (now, before, step, step_before)],
            )

    faces_arrived(0)
    for lanes, (now, before, step, step_before) in differences(0):
        for row, value in enumerate((step, now, step_before, before)):
            pressure_sources[pl.ds(row * 128, 128), lanes] = value

    @pl.loop(0, 4)
    def _(n):
        lanes = pl.ds(pl.multiple_of(n * 256, 256), 256)
        for m in range(2):
            rows = pl.ds(m * 1024, 1024)
            left = jnp.concatenate([weights[kc, rows, :] for kc in (1, 2, 4, 5)], axis=1)
            both = jnp.dot(left, pressure_sources[:, lanes], preferred_element_type=F32)
            product[2 * n, rows, :] = both[:, 0:128]
            product[2 * n + 1, rows, :] = both[:, 128:256]

    faces_arrived(1)
    for lanes, (now, before, step, step_before) in differences(1):
        thickness_sources[pl.ds(0, 128), lanes] = step
        thickness_sources[pl.ds(128, 128), lanes] = step_before

    @pl.loop(0, 4, unroll=4)
    def _(n):
        lanes = pl.ds(pl.multiple_of(n * 256, 256), 256)
        for m in range(2):
            rows = pl.ds(m * 1024, 1024)
            left = jnp.concatenate([weights[kc, rows, :] for kc in (0, 3)], axis=1)
            both = jnp.dot(left, thickness_sources[:, lanes], preferred_element_type=F32)
            for side in range(2):
                slots[pl.ds(m * 1024 * PITCH + 2 * n + side, 1024, stride=PITCH), :] = (
                    product[2 * n + side, rows, :] + both[:, side * 128 : side * 128 + 128]
                )

    back4 = 127 - lax.broadcasted_iota(jnp.int32, (4, 128), 1)
    lane16 = lax.broadcasted_iota(jnp.int32, (16, 128), 1)

    def gather(half, block_x, block_core):
        for n in range(5):
            if n < 4:
                first = (((z + 5 + 2 * n + half) % 8) * 4 + block_x) * 2 + block_core
                for r in range(32):
                    code = table[first, r]
                    row = lax.shift_right_logical(code, 7)
                    turn = code & 127
                    picked = jnp.where(
                        back4 < turn, slots[pl.ds(row, 4), :], slots[pl.ds(row + 1, 4), :]
                    )
                    rows_tmp[n, pl.ds(r * 4, 4), :] = pltpu.roll(picked, turn, 1)
            if n > 0:
                m = n - 1
                chunk = ((z + 5 + 2 * m + half) % 16) // 8
                for j in range(4):
                    top = rows_tmp[m, pl.ds(j, 16, stride=4), :]
                    bottom = rows_tmp[m, pl.ds(64 + j, 16, stride=4), :]
                    yield (
                        (chunk, j, m),
                        jnp.where(lane16 < 64, top, pltpu.roll(bottom, 64, 1)),
                    )
                    yield (
                        (1 - chunk, j, m),
                        jnp.where(lane16 < 64, pltpu.roll(top, 64, 1), bottom),
                    )

    other = 1 - core

    def core_copy(half, chunk):
        return pltpu.make_async_remote_copy(
            src_ref=core_send.at[half, chunk],
            dst_ref=core_recv.at[half, chunk],
            send_sem=core_sems.at[0, half, chunk],
            recv_sem=core_sems.at[1, half, chunk],
            device_id=device(core_=other),
            device_id_type=MESH,
        )

    def spot(half, chunk, xk, j, n):
        return (half, chunk, j, xk, n) if half else (half, chunk, xk, j, n)

    for half in (1, 0):

        @pl.loop(0, 4, unroll=2)
        def _(xk):
            for (chunk, j, n), tile in gather(half, xk, other):
                core_send[spot(half, chunk, xk, j, n)] = tile.astype(BF16)

        for chunk in range(2):
            core_copy(half, chunk).start()

    def copies(stage, half, chunk, k, arriving):
        along_y = half == (stage == 1)
        mine = y if along_y else x
        peer = (mine + (4 - k if arriving else k)) % 4
        source, landing, sems = (send1, recv1, sems1) if stage == 1 else (send2, recv2, sems2)
        return pltpu.make_async_remote_copy(
            src_ref=source.at[half, chunk, peer],
            dst_ref=landing.at[half, chunk, peer if arriving else mine],
            send_sem=sems.at[0, half, chunk, k],
            recv_sem=sems.at[1, half, chunk, k],
            device_id=device(y_=peer) if along_y else device(x_=peer),
            device_id_type=MESH,
        )

    for half in (1, 0):
        for chunk in range(2):
            core_copy(half, chunk).wait_recv()

        @pl.loop(0, 4, unroll=2)
        def _(xk):
            for (chunk, j, n), tile in gather(half, xk, core):
                at = spot(half, chunk, xk, j, n)
                send1[at] = (tile + core_recv[at].astype(F32)).astype(BF16)

        for chunk in range(2):
            for k in (1, 3, 2):
                copies(1, half, chunk, k, False).start()

    def second(half, chunk):
        mine, across = (y, x) if half else (x, y)
        for k in (1, 3, 2):
            copies(1, half, chunk, k, True).wait_recv()
        for k in (2, 1, 3, 0):
            index = (across + k) % 4
            for n in range(4):
                total = send1[half, chunk, mine, index, n].astype(F32)
                for s in range(1, 4):
                    total = total + recv1[half, chunk, (mine + s) % 4, index, n].astype(F32)
                send2[half, chunk, index, n] = total.astype(BF16)
            if k:
                copies(2, half, chunk, k, False).start()

    def copy3(i, arriving):
        dz = (5 + i) % 16
        peer = (z + (16 - dz if arriving else dz)) % 16
        return pltpu.make_async_remote_copy(
            src_ref=send3.at[i],
            dst_ref=recv3.at[i],
            send_sem=sems3.at[0, i],
            recv_sem=sems3.at[1, i],
            device_id=device(z_lo_=peer % 8, z_hi_=peer // 8),
            device_id_type=MESH,
        )

    def third(half, chunk):
        mine = x if half else y
        for k in (1, 3, 2):
            copies(2, half, chunk, k, True).wait_recv()
        for n in ((2, 1, 3, 0), (1, 2, 0, 3))[half]:
            total = send2[half, chunk, mine, n].astype(F32)
            for s in range(1, 4):
                total = total + recv2[half, chunk, (mine + s) % 4, n].astype(F32)
            i = chunk * 8 + 2 * n + half
            send3[i] = total.astype(BF16)
            if i != 11:
                copy3(i, False).start()

    for stage in (second, third):
        for chunk in range(2):
            for half in (1, 0):
                stage(half, chunk)

    total = send3[11].astype(F32)
    for i in (10, 12, 9, 13, 8, 14, 15, 7, 0, 6, 1, 5, 2, 4, 3):
        copy3(i, True).wait_recv()
        total = total + recv3[i].astype(F32)
    out[pl.ds(0, 16), :] = total[:, 0:64]
    out[pl.ds(16, 16), :] = total[:, 64:128]

    for series in range(2):
        pltpu.make_async_copy(
            staging.at[series, pl.ds(0, 63)],
            arrived.at[series, pl.ds(0, 63)],
            face_sems.at[0, series],
        ).wait()
    for half in range(2):
        for chunk in range(2):
            core_copy(half, chunk).wait_send()
            for k in range(1, 4):
                copies(1, half, chunk, k, False).wait_send()
                copies(2, half, chunk, k, False).wait_send()
    for i in range(16):
        if i != 11:
            copy3(i, False).wait_send()


def local(surface_raw, area_normals, kernel_weights, block_map, band_observers, band_lags):
    anywhere = pl.BlockSpec(memory_space=pl.ANY)
    weights = kernel_weights.reshape(6, 2048, 128)
    dma = pltpu.SemaphoreType.DMA
    return pl.pallas_call(
        kernel,
        out_shape=jax.ShapeDtypeStruct((32, 64), F32),
        in_specs=[anywhere] * 6,
        out_specs=pl.BlockSpec(memory_space=pltpu.VMEM),
        scratch_shapes=[
            pltpu.SMEM((1, 1, 64), jnp.int32),
            pltpu.SMEM((16, 128), jnp.int32),
            pltpu.SMEM((16,), jnp.int32),
            pltpu.VMEM((5, 128, 1024), BF16),
            pltpu.VMEM((3, 128), BF16),
            pltpu.VMEM((2, 1024, 128), F32),
            pltpu.VMEM((2, 64, 16, 128), BF16),
            pltpu.VMEM((2, 64, 16, 128), BF16),
            pltpu.VMEM((6, 2048, 128), BF16),
            pltpu.VMEM((512, 1024), BF16),
            pltpu.VMEM((256, 1024), BF16),
            pltpu.VMEM((8, 2048, 128), F32),
            pltpu.VMEM((2048 * PITCH, 128), F32),
            pltpu.VMEM((4, 128, 128), F32),
            pltpu.VMEM((64, 128), jnp.int32),
            pltpu.SMEM((64, 128), jnp.int32),
            pltpu.VMEM((2, 2, 4, 4, 4, 16, 128), BF16),
            pltpu.VMEM((2, 2, 4, 4, 4, 16, 128), BF16),
            pltpu.VMEM((2, 2, 4, 4, 4, 16, 128), BF16),
            pltpu.VMEM((2, 2, 4, 4, 4, 16, 128), BF16),
            pltpu.VMEM((2, 2, 4, 4, 16, 128), BF16),
            pltpu.VMEM((2, 2, 4, 4, 16, 128), BF16),
            pltpu.VMEM((16, 16, 128), BF16),
            pltpu.VMEM((16, 16, 128), BF16),
            pltpu.SemaphoreType.REGULAR((3,)),
            dma((6,)),
            dma,
            dma((2, 2)),
            dma((2, 2, 2)),
            dma((2, 2, 2, 4)),
            dma((2, 2, 2, 4)),
            dma((2, 16)),
        ],
        compiler_params=pltpu.CompilerParams(collective_id=0, has_side_effects=True),
    )(block_map, band_observers, band_lags, surface_raw, area_normals, weights)


def solution(mesh):
    placed = (
        P(None, ("cfd", "ac"), None),
        P(None, ("cfd", "ac")),
        P(None, None, None, ("cfd", "ac")),
        P("ac", "cfd", None),
        P(),
        P(),
    )
    return jax.shard_map(
        local, mesh=mesh, in_specs=placed, out_specs=P("cfd", "ac"), check_vma=False
    )
```
